32 devices in a mesh: dp: 2 (over x), mp: 16 (over z, y, core).
Axes of the slice: x: 2, y: 2, z: 4, core: 2. Of those that a mesh axis runs over, the one named last changes fastest.
Arguments:
- grad_parts: bfloat16 [2, 16, 1, 512, 512], P('dp', 'mp'), may hold values from -0.1875 to 0.1875
- factors: float32 [16, 2, 512, 512], P('mp', 'dp'), may hold values from -1 to 8, as said below
- root_prev: bfloat16 [16, 2, 512, 512], P(None, 'dp', 'mp'), may hold values from -1 to 2, as said below
- plan: int32 [2, 16], P('dp'), may hold values from 0 to 16, as said below
Outputs:
- new_factors: float32 [16, 2, 512, 512], P('mp', 'dp')
- new_roots: bfloat16 [16, 2, 512, 512], P(None, 'dp', 'mp')
The draws below stay inside these ranges and needn't reach their ends.
Inputs may be any that keep to these rules, and one draw needn't show every extreme that they name: In each row of plan no worker is named more than 3 times and one is named exactly 3 times; at least 8 entries of a row are below 16. `factors`: each factor is symmetric. `root_prev`: each root is symmetric.
All inputs are finite; a program needn't handle non-finite values.
Results may differ from the reference program's by a relative error of at most 0.0055.
Values may be sent and summed in bfloat16 or wider, within the bound.
A program may use at most 64 MiB of HBM per device.

```python
import jax
import jax.numpy as jnp
from jax import lax

BS = 512
CAP = 3
HALF = 1
N_DP = 2
N_MP = 16


def spectrum(key):
    upper_end = 4.0
    uniform_draw = jax.random.uniform(jax.random.fold_in(key, 11), (N_MP, N_DP, BS), jnp.float32)
    return 0.5 * jnp.exp(uniform_draw * jnp.log(upper_end / 0.5))


def symmetric(key):
    noise = jax.random.normal(key, (N_MP, N_DP, BS, BS), jnp.float32)
    return (noise + jnp.swapaxes(noise, -1, -2)) * 0.5 ** 0.5


def draw_factors(key, part):
    diagonal_vals = spectrum(key)
    identity = jnp.eye(BS, dtype=jnp.float32)
    outer_scale = jnp.sqrt(diagonal_vals[..., :, None] * diagonal_vals[..., None, :])
    spread = symmetric(jax.random.fold_in(key, 12)) * (0.25 / BS ** 0.5)
    result = outer_scale * spread * (1.0 - identity) + identity * diagonal_vals[..., None, :]
    return result.astype(jnp.float32)


def draw_root_prev(key, part):
    diagonal_vals = spectrum(key)
    identity = jnp.eye(BS, dtype=jnp.float32)
    scaling = diagonal_vals ** (-0.125)
    spread = symmetric(jax.random.fold_in(key, 13)) * (0.2 / BS ** 0.5)
    inner = identity + spread * (1.0 - identity)
    result = scaling[..., :, None] * inner * scaling[..., None, :]
    return result.astype(jnp.bfloat16)


def plan_row(key):
    refreshed = jax.random.randint(jax.random.fold_in(key, 1), (), N_MP // 2, N_MP + 1)
    rank_of = jax.random.permutation(jax.random.fold_in(key, 2), N_MP)
    shuffled = jax.random.permutation(jax.random.fold_in(key, 3), N_MP)
    busiest = shuffled[0]
    remaining = shuffled[1:]
    workers = jnp.concatenate([jnp.full((CAP,), busiest), jnp.full((2,), remaining[0]), remaining[1:]])
    chosen = workers[rank_of]
    return jnp.where(rank_of < refreshed, chosen, N_MP).astype(jnp.int32)


def draw_plan(key, part):
    row_keys = jax.random.split(key, N_DP)
    return jax.vmap(plan_row)(row_keys)


def shard_levels(rng, extent, pieces, smallest, largest):
    level, own = 1.0, jax.random.fold_in(rng, 6)
    for axis_at, shards_of in pieces:
        heights = jnp.exp(jax.random.uniform(jax.random.fold_in(own, axis_at), (shards_of,), jnp.float32, smallest / len(pieces), largest / len(pieces)))
        level = level * jnp.repeat(heights, extent[axis_at] // shards_of).reshape([-1 if axis == axis_at else 1 for axis in range(len(extent))])
    return level


def normal_values(rng, dims, deviation, bound, pieces=(), kind=jnp.bfloat16):
    level = shard_levels(rng, dims, pieces, -0.22, 0.18) if pieces else 1.0
    values = jax.random.normal(rng, dims, jnp.float32) * deviation * level
    return jnp.minimum(jnp.maximum(values, -bound), bound).astype(kind)


def setup_inputs(seed: int = 0) -> dict:
    streams_of = jax.random.split(jax.random.key(seed), 5)
    grad_parts = normal_values(streams_of[0], (N_DP, N_MP, HALF, BS, BS), (BS * N_DP) ** -0.5, 0.1875, ((0, 2), (1, 16)))
    factors = draw_factors(jax.random.fold_in(streams_of[4], 71), 0)
    root_prev = draw_root_prev(jax.random.fold_in(streams_of[4], 71), 0)
    plan = draw_plan(jax.random.fold_in(streams_of[4], 71), 0)
    return dict(grad_parts=grad_parts, factors=factors, root_prev=root_prev, plan=plan)


keep_rate = 0.8


def newton(initial, factor):
    identity = jnp.eye(factor.shape[-1], dtype=jnp.float32)
    square = jnp.einsum("sij,sjk->sik", initial, initial, preferred_element_type=jnp.float32)
    fourth = jnp.einsum("sij,sjk->sik", square, square, precision=lax.Precision.HIGHEST)
    coupled = jnp.einsum("sij,sjk->sik", fourth, factor, precision=lax.Precision.HIGHEST)
    update = (5.0 * identity - coupled) * 0.25
    return jnp.einsum("sij,sjk->sik", initial.astype(jnp.float32), update, precision=lax.Precision.HIGHEST)


def reference(grad_parts, factors, root_prev, plan):
    def per_owner(owner):
        partial_grads = lax.dynamic_index_in_dim(grad_parts, owner, 1, keepdims=False)
        summed = jnp.sum(partial_grads.astype(jnp.float32), axis=0)
        left = jnp.einsum("kij,klj->kil", summed, summed, precision=lax.Precision.HIGHEST)
        right = jnp.einsum("kji,kjl->kil", summed, summed, precision=lax.Precision.HIGHEST)
        grams = jnp.stack([left, right], axis=1).reshape(N_DP, BS, BS)
        old_factor = lax.dynamic_index_in_dim(factors, owner, 0, keepdims=False)
        fresh_factor = keep_rate * old_factor + (1.0 - keep_rate) * grams
        previous = lax.dynamic_index_in_dim(root_prev, owner, 0, keepdims=False)
        refined = newton(previous, fresh_factor).astype(jnp.bfloat16)
        owner_plan = lax.dynamic_index_in_dim(plan, owner, 1, keepdims=False)
        roots = jnp.where(owner_plan[:, None, None] < N_MP, refined, previous)
        return fresh_factor, roots

    new_factors, new_roots = lax.map(per_owner, jnp.arange(N_MP, dtype=jnp.int32))
    return new_factors, new_roots
```

```python
import functools

import jax
import jax.numpy as jnp
from jax import lax
from jax.experimental import pallas as pl
from jax.experimental.pallas import tpu as pltpu
from jax.sharding import PartitionSpec as P

keep_rate = 0.8
MESH = pl.DeviceIdType.MESH
F32 = jnp.float32
BF16 = jnp.bfloat16


def mul(a, b):
    return jnp.dot(a, b, preferred_element_type=F32)


def split(a):
    high = a.astype(BF16)
    return high, (a - high.astype(F32)).astype(BF16)


def kernel(
    n_dp, n_mp, blocks,
    grad, fac, root, fresh, fac_out,
    own_g, in_g, fac_v, root_v, pieces, full_x, rest, fifth, gram_v, out_v, fac_new,
    load_sem, grad_send, grad_recv, root_send, root_recv, out_send, out_recv,
):
    d = lax.axis_index("dp")
    me = lax.axis_index("mp")
    bs = fac.shape[-1]
    half = n_mp // 2
    hb = bs // 2
    side = me // half
    away = 1 - side
    near_cols = pl.ds(pl.multiple_of(side * hb, hb), hb)
    far_cols = pl.ds(pl.multiple_of(away * hb, hb), hb)
    near_pieces = pl.ds(side * half, half)
    far_pieces = pl.ds(away * half, half)

    def far_peer(i):
        return away * half + (me + i) % half

    def near_peer(i):
        return side * half + (me + i) % half

    loads = [
        pltpu.make_async_copy(grad, own_g, load_sem.at[0]),
        pltpu.make_async_copy(root, root_v, load_sem.at[1]),
        pltpu.make_async_copy(root.at[me], pieces.at[me], load_sem.at[2]),
        pltpu.make_async_copy(fac, fac_v, load_sem.at[3]),
    ]
    for load in loads:
        load.start()

    barrier = pltpu.get_barrier_semaphore()

    @pl.loop(1, n_mp)
    def _(i):
        pl.semaphore_signal(barrier, inc=1, device_id=(d, (me + i) % n_mp), device_id_type=MESH)

    for i in range(1, n_dp):
        pl.semaphore_signal(barrier, inc=1, device_id=((d + i) % n_dp, me), device_id_type=MESH)
    pl.semaphore_wait(barrier, n_mp - 1 + n_dp - 1)

    def grad_copy(i):
        other = (d + i) % n_dp
        return pltpu.make_async_remote_copy(
            src_ref=own_g.at[other * blocks // n_dp], dst_ref=in_g.at[i - 1],
            send_sem=grad_send.at[i - 1], recv_sem=grad_recv.at[i - 1],
            device_id=(other, me), device_id_type=MESH,
        )

    loads[0].wait()
    for i in range(1, n_dp):
        grad_copy(i).start()

    def root_far(src, dst, peer, slot, cols):
        return pltpu.make_async_remote_copy(
            src_ref=root_v.at[src, :, cols], dst_ref=pieces.at[dst, :, cols],
            send_sem=root_send.at[peer], recv_sem=root_recv.at[slot],
            device_id=(d, peer), device_id_type=MESH,
        )

    def root_near(src, dst, peer, slot):
        return pltpu.make_async_remote_copy(
            src_ref=root_v.at[src], dst_ref=pieces.at[dst],
            send_sem=root_send.at[peer], recv_sem=root_recv.at[slot],
            device_id=(d, peer), device_id_type=MESH,
        )

    loads[1].wait()

    @pl.loop(0, half)
    def _(i):
        t = far_peer(i)
        root_far(t, me, t, me, near_cols).start()

    @pl.loop(1, half)
    def _(i):
        t = near_peer(i)
        root_near(t, me, t, me).start()

    loads[2].wait()
    loads[3].wait()

    @pl.loop(0, half)
    def _(i):
        s = far_peer(i)
        root_far(s, s, s, s, far_cols).wait_recv()

    @pl.loop(1, half)
    def _(i):
        s = near_peer(i)
        root_near(s, s, s, s).wait_recv()

    near_rows = pieces[near_pieces].astype(F32).reshape(hb, bs).astype(BF16)
    full_x[near_cols, :] = near_rows
    full_x[far_cols, far_cols] = pieces[far_pieces, :, far_cols].astype(F32).reshape(hb, hb).astype(BF16)
    full_x[far_cols, near_cols] = full_x[near_cols, far_cols].astype(F32).T.astype(BF16)

    x = full_x[...]
    sq_h, sq_l = split(mul(x, x))
    fo_h, fo_l = split(mul(sq_h, sq_h) + mul(sq_h, sq_l) + mul(sq_l, sq_h))
    fi_h, fi_l = split(mul(x, fo_h) + mul(x, fo_l))
    fa_h, fa_l = split(fac_v[...])
    fifth[...] = fi_h
    rest[...] = 1.25 * x.astype(F32) - (0.25 * keep_rate) * (
        mul(fi_h, fa_h) + mul(fi_h, fa_l) + mul(fi_l, fa_h)
    )

    for i in range(1, n_dp):
        grad_copy(i).wait_recv()
    total = own_g[d * blocks // n_dp].astype(F32)
    for i in range(1, n_dp):
        total += in_g[i - 1].astype(F32)
    summed = total.astype(BF16)

    @pl.when(d % 2 == 0)
    def _():
        gram_v[...] = lax.dot_general(summed, summed, (((1,), (1,)), ((), ())), preferred_element_type=F32)

    @pl.when(d % 2 == 1)
    def _():
        gram_v[...] = lax.dot_general(summed, summed, (((0,), (0,)), ((), ())), preferred_element_type=F32)

    gram_h = gram_v[...].astype(BF16)

    def out_copy(src, dst, peer, slot):
        return pltpu.make_async_remote_copy(
            src_ref=out_v.at[src], dst_ref=fresh.at[dst],
            send_sem=out_send.at[peer], recv_sem=out_recv.at[slot],
            device_id=(d, peer), device_id_type=MESH,
        )

    def refine(rows, at):
        refined = rest[rows, :] - (0.25 * (1.0 - keep_rate)) * mul(fifth[rows, :], gram_h)
        out_v[at] = refined.reshape(half, bs // n_mp, bs).astype(BF16)

    refine(far_cols, far_pieces)

    @pl.loop(0, half)
    def _(i):
        t = far_peer(i)
        out_copy(t, me, t, me).start()

    refine(near_cols, near_pieces)

    @pl.loop(1, half)
    def _(i):
        t = near_peer(i)
        out_copy(t, me, t, me).start()

    own_out = pltpu.make_async_copy(out_v.at[me], fresh.at[me], load_sem.at[0])
    own_out.start()
    fac_new[...] = keep_rate * fac_v[...] + (1.0 - keep_rate) * gram_v[...]
    fac_store = pltpu.make_async_copy(fac_new, fac_out, load_sem.at[1])
    fac_store.start()

    for i in range(1, n_dp):
        grad_copy(i).wait_send()

    @pl.loop(0, half)
    def _(i):
        t = far_peer(i)
        root_far(t, me, t, me, near_cols).wait_send()

    @pl.loop(1, half)
    def _(i):
        t = near_peer(i)
        root_near(t, me, t, me).wait_send()

    @pl.loop(1, n_mp)
    def _(i):
        s = (me + i) % n_mp
        out_copy(s, s, s, s).wait_send()
        out_copy(s, s, s, s).wait_recv()

    own_out.wait()
    fac_store.wait()


def local(n_dp, n_mp, grad_parts, factors, root_prev, plan):
    blocks, bs = grad_parts.shape[2], factors.shape[-1]
    rows = bs // n_mp
    grads = grad_parts.reshape(blocks, bs, bs)
    old = root_prev.reshape(n_mp, rows, bs)
    fresh, new_factor = pl.pallas_call(
        functools.partial(kernel, n_dp, n_mp, blocks),
        out_shape=(
            jax.ShapeDtypeStruct((n_mp, rows, bs), BF16),
            jax.ShapeDtypeStruct((bs, bs), F32),
        ),
        in_specs=[pl.BlockSpec(memory_space=pl.ANY)] * 3,
        out_specs=(pl.BlockSpec(memory_space=pl.ANY),) * 2,
        scratch_shapes=[
            pltpu.VMEM((blocks, bs, bs), BF16),
            pltpu.VMEM((n_dp - 1, bs, bs), BF16),
            pltpu.VMEM((bs, bs), F32),
            pltpu.VMEM((n_mp, rows, bs), BF16),
            pltpu.VMEM((n_mp, rows, bs), BF16),
            pltpu.VMEM((bs, bs), BF16),
            pltpu.VMEM((bs, bs), F32),
            pltpu.VMEM((bs, bs), BF16),
            pltpu.VMEM((bs, bs), F32),
            pltpu.VMEM((n_mp, rows, bs), BF16),
            pltpu.VMEM((bs, bs), F32),
            pltpu.SemaphoreType.DMA((4,)),
            pltpu.SemaphoreType.DMA((n_dp - 1,)),
            pltpu.SemaphoreType.DMA((n_dp - 1,)),
            pltpu.SemaphoreType.DMA((n_mp,)),
            pltpu.SemaphoreType.DMA((n_mp,)),
            pltpu.SemaphoreType.DMA((n_mp,)),
            pltpu.SemaphoreType.DMA((n_mp,)),
        ],
        compiler_params=pltpu.CompilerParams(collective_id=0, has_side_effects=True),
        name="refresh",
    )(grads, factors.reshape(bs, bs), old)
    refresh = plan[0] < n_mp
    new_roots = jnp.where(refresh[:, None, None], fresh, old).reshape(root_prev.shape)
    return (new_factor[None, None], new_roots)


def solution(mesh):
    return jax.shard_map(
        functools.partial(local, mesh.shape["dp"], mesh.shape["mp"]),
        mesh=mesh,
        in_specs=(
            P("dp", "mp", None, None, None),
            P("mp", "dp", None, None),
            P(None, "dp", "mp", None),
            P("dp", None),
        ),
        out_specs=(P("mp", "dp", None, None), P(None, "dp", "mp", None)),
        check_vma=False,
    )
```

```python
import functools

import jax
import jax.numpy as jnp
from jax import lax
from jax.experimental import pallas as pl
from jax.experimental.pallas import tpu as pltpu
from jax.sharding import PartitionSpec as P

keep_rate = 0.8
MESH = pl.DeviceIdType.MESH
F32 = jnp.float32
BF16 = jnp.bfloat16


def mul(a, b):
    return jnp.dot(a, b, preferred_element_type=F32)


def split(a):
    high = a.astype(BF16)
    return high, (a - high.astype(F32)).astype(BF16)


def kernel(
    n_dp, n_mp, blocks,
    plan, grad, fac, root, fresh, fac_out,
    own_g, in_g, fac_v, root_v, pieces, full_x, rest, fifth, gram_v, out_v,
    load_sem, grad_send, grad_recv, root_send, root_recv, out_send, out_recv, turn,
):
    d = lax.axis_index("dp")
    me = lax.axis_index("mp")
    bs = fac.shape[-1]
    half = n_mp // 2
    hb = bs // 2
    side = me // half
    away = 1 - side
    near_cols = pl.ds(pl.multiple_of(side * hb, hb), hb)
    far_cols = pl.ds(pl.multiple_of(away * hb, hb), hb)
    near_pieces = pl.ds(side * half, half)
    far_pieces = pl.ds(away * half, half)

    def far_peer(i):
        return away * half + (me + i) % half

    def near_peer(i):
        return side * half + (me + i) % half

    loads = [
        pltpu.make_async_copy(grad, own_g, load_sem.at[0]),
        pltpu.make_async_copy(root, root_v, load_sem.at[1]),
        pltpu.make_async_copy(root.at[me], pieces.at[me], load_sem.at[2]),
        pltpu.make_async_copy(fac, fac_v, load_sem.at[3]),
    ]
    for load in loads:
        load.start()

    barrier = pltpu.get_barrier_semaphore()

    @pl.loop(1, n_mp)
    def _(i):
        pl.semaphore_signal(barrier, inc=1, device_id=(d, (me + i) % n_mp), device_id_type=MESH)

    for i in range(1, n_dp):
        pl.semaphore_signal(barrier, inc=1, device_id=((d + i) % n_dp, me), device_id_type=MESH)
    pl.semaphore_wait(barrier, n_mp - 1 + n_dp - 1)

    def grad_copy(i):
        other = (d + i) % n_dp
        return pltpu.make_async_remote_copy(
            src_ref=own_g.at[other * blocks // n_dp], dst_ref=in_g.at[i - 1],
            send_sem=grad_send.at[i - 1], recv_sem=grad_recv.at[i - 1],
            device_id=(other, me), device_id_type=MESH,
        )

    loads[0].wait()
    lead = me % 2 == 0

    @pl.when(lead)
    def _():
        for i in range(1, n_dp):
            grad_copy(i).start()

    def root_far(src, dst, peer, slot, cols):
        return pltpu.make_async_remote_copy(
            src_ref=root_v.at[src, :, cols], dst_ref=pieces.at[dst, :, cols],
            send_sem=root_send.at[peer], recv_sem=root_recv.at[slot],
            device_id=(d, peer), device_id_type=MESH,
        )

    def root_near(src, dst, peer, slot):
        return pltpu.make_async_remote_copy(
            src_ref=root_v.at[src], dst_ref=pieces.at[dst],
            send_sem=root_send.at[peer], recv_sem=root_recv.at[slot],
            device_id=(d, peer), device_id_type=MESH,
        )

    loads[1].wait()

    for parity in range(2):
        @pl.loop(0, half // 2)
        def _(i):
            t = away * half + (me // 2 * 2 + 2 * i) % half + parity
            root_far(t, me, t, me, near_cols).start()

        @pl.loop(0, half // 2)
        def _(i):
            t = side * half + (me // 2 * 2 + 2 * i) % half + parity

            @pl.when(t != me)
            def _():
                root_near(t, me, t, me).start()

    @pl.when(lead)
    def _():
        for i in range(1, n_dp):
            grad_copy(i).wait_send()
        pl.semaphore_signal(turn, inc=1, device_id=(d, me + 1), device_id_type=MESH)

    @pl.when(jnp.logical_not(lead))
    def _():
        pl.semaphore_wait(turn, 1)
        for i in range(1, n_dp):
            grad_copy(i).start()

    loads[2].wait()
    loads[3].wait()

    @pl.loop(0, half)
    def _(i):
        s = far_peer(i)
        root_far(s, s, s, s, far_cols).wait_recv()

    @pl.loop(1, half)
    def _(i):
        s = near_peer(i)
        root_near(s, s, s, s).wait_recv()

    near_rows = pieces[near_pieces].astype(F32).reshape(hb, bs).astype(BF16)
    full_x[near_cols, :] = near_rows
    full_x[far_cols, far_cols] = pieces[far_pieces, :, far_cols].astype(F32).reshape(hb, hb).astype(BF16)
    full_x[far_cols, near_cols] = full_x[near_cols, far_cols].astype(F32).T.astype(BF16)

    x = full_x[...]
    sq_h, sq_l = split(mul(x, x))
    fourth = (mul(sq_h, sq_h) + mul(sq_h, sq_l) + mul(sq_l, sq_h)).astype(BF16)
    fifth[...] = mul(x, fourth).astype(BF16)
    rest[...] = 1.25 * x.astype(F32) - (0.25 * keep_rate) * mul(fifth[...], fac_v[...].astype(BF16))

    for i in range(1, n_dp):
        grad_copy(i).wait_recv()
    total = own_g[d * blocks // n_dp].astype(F32)
    for i in range(1, n_dp):
        total += in_g[i - 1].astype(F32)
    summed = total.astype(BF16)

    @pl.when(d % 2 == 0)
    def _():
        gram_v[...] = lax.dot_general(summed, summed, (((1,), (1,)), ((), ())), preferred_element_type=F32)

    @pl.when(d % 2 == 1)
    def _():
        gram_v[...] = lax.dot_general(summed, summed, (((0,), (0,)), ((), ())), preferred_element_type=F32)

    gram_h = gram_v[...].astype(BF16)

    def out_copy(src, dst, peer, slot):
        return pltpu.make_async_remote_copy(
            src_ref=out_v.at[src], dst_ref=fresh.at[dst],
            send_sem=out_send.at[peer], recv_sem=out_recv.at[slot],
            device_id=(d, peer), device_id_type=MESH,
        )

    kept = plan[0, me] >= n_mp

    def refine(rows, at):
        refined = rest[rows, :] - (0.25 * (1.0 - keep_rate)) * mul(fifth[rows, :], gram_h)
        refined = jnp.where(kept, full_x[rows, :].astype(F32), refined)
        out_v[at] = refined.reshape(half, bs // n_mp, bs).astype(BF16)

    refine(far_cols, far_pieces)

    @pl.loop(0, half)
    def _(i):
        t = far_peer(i)
        out_copy(t, me, t, me).start()

    refine(near_cols, near_pieces)

    @pl.loop(1, half)
    def _(i):
        t = near_peer(i)
        out_copy(t, me, t, me).start()

    own_out = pltpu.make_async_copy(out_v.at[me], fresh.at[me], load_sem.at[0])
    own_out.start()
    fac_out[...] = keep_rate * fac_v[...] + (1.0 - keep_rate) * gram_v[...]

    @pl.when(jnp.logical_not(lead))
    def _():
        for i in range(1, n_dp):
            grad_copy(i).wait_send()

    @pl.loop(0, half)
    def _(i):
        t = far_peer(i)
        root_far(t, me, t, me, near_cols).wait_send()

    @pl.loop(1, half)
    def _(i):
        t = near_peer(i)
        root_near(t, me, t, me).wait_send()

    @pl.loop(1, n_mp)
    def _(i):
        s = (me + i) % n_mp
        out_copy(s, s, s, s).wait_send()
        out_copy(s, s, s, s).wait_recv()

    own_out.wait()


def local(n_dp, n_mp, grad_parts, factors, root_prev, plan):
    blocks, bs = grad_parts.shape[2], factors.shape[-1]
    rows = bs // n_mp
    grads = grad_parts.reshape(blocks, bs, bs)
    old = root_prev.reshape(n_mp, rows, bs)
    fresh, new_factor = pl.pallas_call(
        functools.partial(kernel, n_dp, n_mp, blocks),
        out_shape=(
            pltpu.VMEM((n_mp, rows, bs), BF16),
            pltpu.VMEM((bs, bs), F32),
        ),
        in_specs=[pl.BlockSpec(memory_space=pltpu.SMEM)] + [pl.BlockSpec(memory_space=pl.ANY)] * 3,
        out_specs=(pl.BlockSpec(memory_space=pltpu.VMEM),) * 2,
        scratch_shapes=[
            pltpu.VMEM((blocks, bs, bs), BF16),
            pltpu.VMEM((n_dp - 1, bs, bs), BF16),
            pltpu.VMEM((bs, bs), F32),
            pltpu.VMEM((n_mp, rows, bs), BF16),
            pltpu.VMEM((n_mp, rows, bs), BF16),
            pltpu.VMEM((bs, bs), BF16),
            pltpu.VMEM((bs, bs), F32),
            pltpu.VMEM((bs, bs), BF16),
            pltpu.VMEM((bs, bs), F32),
            pltpu.VMEM((n_mp, rows, bs), BF16),
            pltpu.SemaphoreType.DMA((4,)),
            pltpu.SemaphoreType.DMA((n_dp - 1,)),
            pltpu.SemaphoreType.DMA((n_dp - 1,)),
            pltpu.SemaphoreType.DMA((n_mp,)),
            pltpu.SemaphoreType.DMA((n_mp,)),
            pltpu.SemaphoreType.DMA((n_mp,)),
            pltpu.SemaphoreType.DMA((n_mp,)),
            pltpu.SemaphoreType.REGULAR,
        ],
        compiler_params=pltpu.CompilerParams(collective_id=0, has_side_effects=True),
        name="refresh",
    )(plan, grads, factors.reshape(bs, bs), old)
    return (new_factor[None, None], fresh.reshape(root_prev.shape))


def solution(mesh):
    return jax.shard_map(
        functools.partial(local, mesh.shape["dp"], mesh.shape["mp"]),
        mesh=mesh,
        in_specs=(
            P("dp", "mp", None, None, None),
            P("mp", "dp", None, None),
            P(None, "dp", "mp", None),
            P("dp", None),
        ),
        out_specs=(P("mp", "dp", None, None), P(None, "dp", "mp", None)),
        check_vma=False,
    )
```

```python
import functools

import jax
import jax.numpy as jnp
from jax import lax
from jax.experimental import pallas as pl
from jax.experimental.pallas import tpu as pltpu
from jax.sharding import PartitionSpec as P

keep_rate = 0.8
MESH = pl.DeviceIdType.MESH
F32 = jnp.float32
BF16 = jnp.bfloat16


def mul(a, b):
    return jnp.dot(a, b, preferred_element_type=F32)


def split(a):
    high = a.astype(BF16)
    return high, (a - high.astype(F32)).astype(BF16)


def kernel(
    n_dp, n_mp, blocks,
    plan, grad, fac, root, fresh, fac_out, plan_s,
    own_g, in_g, fac_v, root_v, pieces, full_x, rest, fifth, gram_v, out_v,
    load_sem, grad_send, grad_recv, root_send, root_recv, out_send, out_recv, turn,
):
    d = lax.axis_index("dp")
    me = lax.axis_index("mp")
    bs = fac.shape[-1]
    half = n_mp // 2
    hb = bs // 2
    side = me // half
    away = 1 - side
    near_cols = pl.ds(pl.multiple_of(side * hb, hb), hb)
    far_cols = pl.ds(pl.multiple_of(away * hb, hb), hb)
    near_pieces = pl.ds(side * half, half)
    far_pieces = pl.ds(away * half, half)

    def far_peer(i):
        return away * half + (me + i) % half

    def near_peer(i):
        return side * half + (me + i) % half

    loads = [
        pltpu.make_async_copy(grad, own_g, load_sem.at[0]),
        pltpu.make_async_copy(root, root_v, load_sem.at[1]),
        pltpu.make_async_copy(root.at[me], pieces.at[me], load_sem.at[2]),
        pltpu.make_async_copy(fac, fac_v, load_sem.at[3]),
        pltpu.make_async_copy(plan, plan_s, load_sem.at[4]),
    ]
    for load in loads:
        load.start()

    barrier = pltpu.get_barrier_semaphore()

    @pl.loop(1, n_mp)
    def _(i):
        pl.semaphore_signal(barrier, inc=1, device_id=(d, (me + i) % n_mp), device_id_type=MESH)

    for i in range(1, n_dp):
        pl.semaphore_signal(barrier, inc=1, device_id=((d + i) % n_dp, me), device_id_type=MESH)
    pl.semaphore_wait(barrier, n_mp - 1 + n_dp - 1)

    def grad_copy(i):
        other = (d + i) % n_dp
        return pltpu.make_async_remote_copy(
            src_ref=own_g.at[other * blocks // n_dp], dst_ref=in_g.at[i - 1],
            send_sem=grad_send.at[i - 1], recv_sem=grad_recv.at[i - 1],
            device_id=(other, me), device_id_type=MESH,
        )

    loads[0].wait()
    lead = me % 2 == 0

    @pl.when(lead)
    def _():
        for i in range(1, n_dp):
            grad_copy(i).start()

    def root_far(src, dst, peer, slot, cols):
        return pltpu.make_async_remote_copy(
            src_ref=root_v.at[src, :, cols], dst_ref=pieces.at[dst, :, cols],
            send_sem=root_send.at[peer], recv_sem=root_recv.at[slot],
            device_id=(d, peer), device_id_type=MESH,
        )

    def root_near(src, dst, peer, slot):
        return pltpu.make_async_remote_copy(
            src_ref=root_v.at[src], dst_ref=pieces.at[dst],
            send_sem=root_send.at[peer], recv_sem=root_recv.at[slot],
            device_id=(d, peer), device_id_type=MESH,
        )

    loads[1].wait()

    for parity in range(2):
        @pl.loop(0, half // 2)
        def _(i):
            t = away * half + (me // 2 * 2 + 2 * i) % half + parity
            root_far(t, me, t, me, near_cols).start()

        @pl.loop(0, half // 2)
        def _(i):
            t = side * half + (me // 2 * 2 + 2 * i) % half + parity

            @pl.when(t != me)
            def _():
                root_near(t, me, t, me).start()

    @pl.when(lead)
    def _():
        for i in range(1, n_dp):
            grad_copy(i).wait_send()
        pl.semaphore_signal(turn, inc=1, device_id=(d, me + 1), device_id_type=MESH)

    @pl.when(jnp.logical_not(lead))
    def _():
        pl.semaphore_wait(turn, 1)
        for i in range(1, n_dp):
            grad_copy(i).start()

    loads[2].wait()
    loads[3].wait()

    @pl.loop(0, half)
    def _(i):
        s = far_peer(i)
        root_far(s, s, s, s, far_cols).wait_recv()

    @pl.loop(1, half)
    def _(i):
        s = near_peer(i)
        root_near(s, s, s, s).wait_recv()

    near_rows = pieces[near_pieces].astype(F32).reshape(hb, bs).astype(BF16)
    full_x[near_cols, :] = near_rows
    full_x[far_cols, far_cols] = pieces[far_pieces, :, far_cols].astype(F32).reshape(hb, hb).astype(BF16)
    full_x[far_cols, near_cols] = full_x[near_cols, far_cols].astype(F32).T.astype(BF16)

    x = full_x[...]
    sq_h, sq_l = split(mul(x, x))
    fourth = (mul(sq_h, sq_h) + mul(sq_h, sq_l) + mul(sq_l, sq_h)).astype(BF16)
    fifth[...] = mul(x, fourth).astype(BF16)
    rest[...] = 1.25 * x.astype(F32) - (0.25 * keep_rate) * mul(fifth[...], fac_v[...].astype(BF16))

    for i in range(1, n_dp):
        grad_copy(i).wait_recv()
    total = own_g[d * blocks // n_dp].astype(F32)
    for i in range(1, n_dp):
        total += in_g[i - 1].astype(F32)
    summed = total.astype(BF16)

    @pl.when(d % 2 == 0)
    def _():
        gram_v[...] = lax.dot_general(summed, summed, (((1,), (1,)), ((), ())), preferred_element_type=F32)

    @pl.when(d % 2 == 1)
    def _():
        gram_v[...] = lax.dot_general(summed, summed, (((0,), (0,)), ((), ())), preferred_element_type=F32)

    gram_h = gram_v[...].astype(BF16)

    def out_copy(src, dst, peer, slot):
        return pltpu.make_async_remote_copy(
            src_ref=out_v.at[src], dst_ref=fresh.at[dst],
            send_sem=out_send.at[peer], recv_sem=out_recv.at[slot],
            device_id=(d, peer), device_id_type=MESH,
        )

    loads[4].wait()
    kept = plan_s[0, me] >= n_mp

    def refine(rows, at):
        refined = rest[rows, :] - (0.25 * (1.0 - keep_rate)) * mul(fifth[rows, :], gram_h)
        refined = jnp.where(kept, full_x[rows, :].astype(F32), refined)
        out_v[at] = refined.reshape(half, bs // n_mp, bs).astype(BF16)

    refine(far_cols, far_pieces)

    @pl.loop(0, half)
    def _(i):
        t = far_peer(i)
        out_copy(t, me, t, me).start()

    refine(near_cols, near_pieces)

    @pl.loop(1, half)
    def _(i):
        t = near_peer(i)
        out_copy(t, me, t, me).start()

    own_out = pltpu.make_async_copy(out_v.at[me], fresh.at[me], load_sem.at[0])
    own_out.start()
    fac_out[...] = keep_rate * fac_v[...] + (1.0 - keep_rate) * gram_v[...]

    @pl.when(jnp.logical_not(lead))
    def _():
        for i in range(1, n_dp):
            grad_copy(i).wait_send()

    @pl.loop(0, half)
    def _(i):
        t = far_peer(i)
        root_far(t, me, t, me, near_cols).wait_send()

    @pl.loop(1, half)
    def _(i):
        t = near_peer(i)
        root_near(t, me, t, me).wait_send()

    @pl.loop(1, n_mp)
    def _(i):
        s = (me + i) % n_mp
        out_copy(s, s, s, s).wait_send()
        out_copy(s, s, s, s).wait_recv()

    own_out.wait()


def local(n_dp, n_mp, grad_parts, factors, root_prev, plan):
    blocks, bs = grad_parts.shape[2], factors.shape[-1]
    rows = bs // n_mp
    grads = grad_parts.reshape(blocks, bs, bs)
    old = root_prev.reshape(n_mp, rows, bs)
    fresh, new_factor = pl.pallas_call(
        functools.partial(kernel, n_dp, n_mp, blocks),
        out_shape=(
            pltpu.VMEM((n_mp, rows, bs), BF16),
            pltpu.VMEM((bs, bs), F32),
        ),
        in_specs=[pl.BlockSpec(memory_space=pl.ANY)] * 4,
        out_specs=(pl.BlockSpec(memory_space=pltpu.VMEM),) * 2,
        scratch_shapes=[
            pltpu.SMEM(plan.shape, plan.dtype),
            pltpu.VMEM((blocks, bs, bs), BF16),
            pltpu.VMEM((n_dp - 1, bs, bs), BF16),
            pltpu.VMEM((bs, bs), F32),
            pltpu.VMEM((n_mp, rows, bs), BF16),
            pltpu.VMEM((n_mp, rows, bs), BF16),
            pltpu.VMEM((bs, bs), BF16),
            pltpu.VMEM((bs, bs), F32),
            pltpu.VMEM((bs, bs), BF16),
            pltpu.VMEM((bs, bs), F32),
            pltpu.VMEM((n_mp, rows, bs), BF16),
            pltpu.SemaphoreType.DMA((5,)),
            pltpu.SemaphoreType.DMA((n_dp - 1,)),
            pltpu.SemaphoreType.DMA((n_dp - 1,)),
            pltpu.SemaphoreType.DMA((n_mp,)),
            pltpu.SemaphoreType.DMA((n_mp,)),
            pltpu.SemaphoreType.DMA((n_mp,)),
            pltpu.SemaphoreType.DMA((n_mp,)),
            pltpu.SemaphoreType.REGULAR,
        ],
        compiler_params=pltpu.CompilerParams(collective_id=0, has_side_effects=True),
        name="refresh",
    )(plan, grads, factors.reshape(bs, bs), old)
    return (new_factor[None, None], fresh.reshape(root_prev.shape))


def solution(mesh):
    return jax.shard_map(
        functools.partial(local, mesh.shape["dp"], mesh.shape["mp"]),
        mesh=mesh,
        in_specs=(
            P("dp", "mp", None, None, None),
            P("mp", "dp", None, None),
            P(None, "dp", "mp", None),
            P("dp", None),
        ),
        out_specs=(P("mp", "dp", None, None), P(None, "dp", "mp", None)),
        check_vma=False,
    )
```
